16 devices in a mesh: dp: 1, sp: 16 (over x, y, z, core).
Axes of the slice: x: 2, y: 2, z: 2, core: 2. Of those that a mesh axis runs over, the one named last changes fastest.
Arguments:
- x: bfloat16 [2048, 12288], P(('dp', 'sp'))
- gain: bfloat16 [12288], replicated
- wq: bfloat16 [12288, 12288], replicated
- wk: bfloat16 [12288, 12288], replicated
- wv: bfloat16 [12288, 12288], replicated
- wo: bfloat16 [12288, 12288], replicated
Outputs:
- output: bfloat16 [2048, 12288], P(('dp', 'sp'))
All inputs are finite; a program needn't handle non-finite values.
Results may differ from the reference program's by a relative error of at most 0.012.
Values are sent between devices in bfloat16 or wider.
A program may use at most 2.75 GiB of HBM per device.

```python
import jax
import jax.numpy as jnp
from jax import lax

ROWS = 2048
D = 12288
HEADS = 96
KV_HEADS = 96
HEAD = 128
THETA = 10000


def setup_inputs(seed: int = 0, part: int = 0) -> dict:
    kx, kn, kq, kk, kv, ko = jax.random.split(jax.random.key(seed), 6)

    def weights(key, rows, columns):
        return jax.random.normal(key, (rows, columns), jnp.float32) * rows**-0.5

    drawn = {
        "x": jax.random.normal(jax.random.fold_in(kx, part), (ROWS, D), jnp.float32),
        "gain": 1 + 0.1 * jax.random.normal(kn, (D,), jnp.float32),
        "wq": 2 * weights(kq, D, HEADS * HEAD),
        "wk": 2 * weights(kk, D, KV_HEADS * HEAD),
        "wv": 4 * weights(kv, D, KV_HEADS * HEAD),
        "wo": weights(ko, HEADS * HEAD, D),
    }
    return {k: v.astype(jnp.bfloat16) for k, v in drawn.items()}


def normed(x, gain):
    wide = x.astype(jnp.float32)
    scale = lax.rsqrt(jnp.mean(wide * wide, -1, keepdims=True) + 1e-6)
    return (wide * scale * gain.astype(jnp.float32)).astype(jnp.bfloat16)


def turned(t, place, theta):
    half = t.shape[-1] // 2
    angle = place.astype(jnp.float32)[:, None] * theta ** (-jnp.arange(half, dtype=jnp.float32) / half)
    cos, sin = jnp.cos(angle)[:, None], jnp.sin(angle)[:, None]
    a, b = t[..., :half].astype(jnp.float32), t[..., half:].astype(jnp.float32)
    return jnp.concatenate([a * cos - b * sin, b * cos + a * sin], -1).astype(jnp.bfloat16)


def matmul(a, w):
    return jnp.dot(a, w, preferred_element_type=jnp.float32).astype(jnp.bfloat16)


def einsum(form, a, b):
    return jnp.einsum(form, a.astype(jnp.float32), b.astype(jnp.float32))


def attention(q, k, v):
    scores = einsum("tgsd,ugd->gstu", q, k) * q.shape[-1] ** -0.5
    token = jnp.arange(q.shape[0])
    scores = jnp.where(token[:, None] >= token, scores, -jnp.inf)
    weights = jax.nn.softmax(scores, -1).astype(jnp.bfloat16)
    return einsum("gstu,ugd->tgsd", weights, v).astype(jnp.bfloat16)


def reference(x, gain, wq, wk, wv, wo):
    a, place = normed(x, gain), jnp.arange(ROWS)
    q = turned(matmul(a, wq).reshape(ROWS, HEADS, HEAD), place, THETA).reshape(ROWS, KV_HEADS, -1, HEAD)
    k = turned(matmul(a, wk).reshape(ROWS, KV_HEADS, HEAD), place, THETA)
    v = matmul(a, wv).reshape(ROWS, KV_HEADS, HEAD)
    seen = attention(q, k, v).reshape(ROWS, HEADS * HEAD)
    return (x.astype(jnp.float32) + jnp.dot(seen, wo, preferred_element_type=jnp.float32)).astype(jnp.bfloat16)
```

```python
import functools

import jax
import jax.numpy as jnp
from jax import lax
from jax.experimental import pallas as pl
from jax.experimental.pallas import tpu as pltpu
from jax.sharding import PartitionSpec as P


HEAD = 128
THETA = 10000
NEG = -1e30
HIDDEN = 2 * NEG
LOG2E = 1.4426950408889634

D = 12288
OWN = 128
TOK = 256
SEQ = 2048
CHIPS = 8
HEADS = 6
W = HEADS * HEAD
BLK = 2 * W
KB = D // BLK
GROUPS = 12
OUTS = D // BLK
RING = 5
BLOCKS = GROUPS * KB + OUTS * 4
LAG = 32

ORDER = (7, 1, 6, 2, 5, 4, 3, 0)


def _xor(a, b):
    out = 0
    for bit in (1, 2, 4):
        p, q = lax.rem(lax.div(a, bit), 2), lax.rem(lax.div(b, bit), 2)
        out = out + bit * (p + q - 2 * p * q)
    return out


def _mask(core, p):
    m, j = lax.div(p, 4), lax.rem(p, 4)
    jj = 3 - j
    even = 6 - lax.div(jj * (jj + 1), 2)
    odd = lax.rem(core + m, 2)
    return even + odd * (7 - 2 * even)


def _pick(table, k):
    out = 0
    for i, v in enumerate(table):
        out = out + jnp.where(k == i, v, 0)
    return out


def _dot(a, b, ca, cb):
    return lax.dot_general(a, b, (((ca,), (cb,)), ((), ())), preferred_element_type=jnp.float32)


def attend_block(q_ref, k_ref, vt_ref, top_s, mix_s, iq):
    e = HEAD**-0.5 * LOG2E
    rows = pl.ds(pl.multiple_of(iq * TOK, TOK), TOK)
    top_s[...] = jnp.full(top_s.shape, NEG, jnp.float32)
    mix_s[...] = jnp.zeros(mix_s.shape, jnp.float32)

    def block(start, size, masked):
        here = pl.ds(pl.multiple_of(start, TOK), size)
        ones = jnp.ones((8, size), jnp.bfloat16)
        scores = [_dot(k_ref[here, h * HEAD : (h + 1) * HEAD], q_ref[rows, h * HEAD : (h + 1) * HEAD], 1, 1) for h in range(HEADS)]
        if masked:
            ok = lax.broadcasted_iota(jnp.int32, (size, TOK), 0) <= lax.broadcasted_iota(jnp.int32, (size, TOK), 1)
        weights, keeps = [], []
        for h, s in enumerate(scores):
            if masked:
                s = jnp.where(ok, s, HIDDEN)
            old = top_s[h : h + 1, :]
            top = jnp.maximum(old, s.max(axis=0, keepdims=True))
            top_s[h : h + 1, :] = top
            weights.append(jnp.exp2((s - top) * e).astype(jnp.bfloat16))
            keeps.append(jnp.exp2((old - top) * e))
        for h, (p, keep) in enumerate(zip(weights, keeps)):
            values = jnp.concatenate([vt_ref[h * HEAD : (h + 1) * HEAD, here], ones], axis=0)
            mix_s[h] = mix_s[h] * keep + _dot(values, p, 1, 0)

    lax.fori_loop(0, lax.div(iq, 2), lambda j, _: block(j * 2 * TOK, 2 * TOK, False), None)

    @pl.when(lax.rem(iq, 2) == 1)
    def _():
        block((iq - 1) * TOK, TOK, False)

    block(iq * TOK, TOK, True)
    for h in range(HEADS):
        q_ref[rows, h * HEAD : (h + 1) * HEAD] = (mix_s[h, :HEAD, :] * (1 / mix_s[h, HEAD : HEAD + 1, :])).T.astype(jnp.bfloat16)


def layer(x_ref, gain_ref, cos_ref, sin_ref, wq_ref, wk_ref, wv_ref, wo_ref, y_ref,
          a_s, q_s, k_s, vt_s, wbuf, acc, stage, vstage, seen, other, xbuf, top_s, mix_s,
          w_sem, x_sem, a_send, a_recv, s_send, s_recv, o_send, o_recv, p_send, p_recv, y_sem):
    me = lax.axis_index("sp")
    chip, core = lax.div(me, 2), lax.rem(me, 2)
    partner = me + 1 - 2 * core

    def to(d):
        return dict(device_id={"sp": d}, device_id_type=pl.DeviceIdType.MESH)

    def slot_of(i):
        return lax.rem(i, RING)

    def source(k):
        return _xor(chip, _pick(ORDER, k))

    def fetch(i):
        slot = slot_of(i)

        def column(w_ref, p):
            cols = pl.ds(pl.multiple_of(_xor(chip, _mask(core, p)) * BLK, BLK), BLK)
            rows = pl.ds(pl.multiple_of(lax.rem(i, KB) * BLK, BLK), BLK)
            pltpu.make_async_copy(w_ref.at[rows, cols], wbuf.at[slot], w_sem.at[slot]).start()

        p = lax.div(i, KB)
        for m, w_ref in enumerate((wq_ref, wk_ref, wv_ref)):
            @pl.when((p >= 4 * m) & (p < 4 * m + 4))
            def _():
                column(w_ref, p)

        @pl.when((i >= GROUPS * KB) & (i < BLOCKS))
        def _():
            n, b = lax.div(i - GROUPS * KB, 4), lax.rem(i, 4)
            cols = pl.ds(pl.multiple_of(n * BLK, BLK), BLK)
            for half in range(2):
                rows = pl.ds(pl.multiple_of((2 * source(2 * b + half) + core) * W, W), W)
                pltpu.make_async_copy(wo_ref.at[rows, cols], wbuf.at[slot, half * W : (half + 1) * W, :], w_sem.at[slot]).start()

    def arrived(i):
        slot = slot_of(i)
        pltpu.make_async_copy(wq_ref.at[:BLK, :BLK], wbuf.at[slot], w_sem.at[slot]).wait()
        return wbuf[slot]

    x_in = pltpu.make_async_copy(x_ref, xbuf, x_sem)
    x_in.start()
    for i in range(RING):
        fetch(jnp.int32(i))

    barrier = pltpu.get_barrier_semaphore()
    for step in range(1, 16):
        pl.semaphore_signal(barrier, inc=1, **to(lax.rem(me + step, 16)))
    pl.semaphore_wait(barrier, 15)

    x_in.wait()

    def a_copy(r):
        rows = pl.ds(pl.multiple_of(core * OWN + r * LAG, LAG), LAG)
        return pltpu.make_async_remote_copy(a_s.at[rows, :], a_s.at[rows, :], a_send.at[r], a_recv.at[r], **to(partner))

    for r in range(OWN // LAG):
        wide = xbuf[r * LAG : (r + 1) * LAG, :].astype(jnp.float32)
        scale = lax.rsqrt(jnp.mean(wide * wide, -1, keepdims=True) + 1e-6)
        rows = pl.ds(pl.multiple_of(core * OWN + r * LAG, LAG), LAG)
        a_s[rows, :] = (wide * scale * gain_ref[...].astype(jnp.float32)).astype(jnp.bfloat16)
        if r:
            a_copy(r - 1).start()
    a_copy(OWN // LAG - 1).start()
    for r in range(OWN // LAG):
        rows = pl.ds(pl.multiple_of((1 - core) * OWN + r * LAG, LAG), LAG)
        pltpu.make_async_remote_copy(a_s.at[rows, :], a_s.at[rows, :], a_send.at[r], a_recv.at[r], **to(partner)).wait_recv()

    def place(m, ref, half, slot):
        if m == 2:
            return vstage.at[slot, half * W : (half + 1) * W, :], vt_s.at[:, pl.ds(pl.multiple_of(ref * TOK, TOK), TOK)]
        return (stage.at[slot, :, half * W : (half + 1) * W], (q_s, k_s)[m].at[pl.ds(pl.multiple_of(ref * TOK, TOK), TOK), :])

    def send(p):
        slot = lax.rem(p, 2)
        t = _xor(chip, _mask(core, p))
        for m in range(3):
            @pl.when((p >= 4 * m) & (p < 4 * m + 4))
            def _():
                for half in range(2):
                    src, dst = place(m, chip, half, slot)
                    owner = 2 * t + half

                    @pl.when(owner == me)
                    def _():
                        pltpu.make_async_copy(src, dst, s_recv.at[m, chip]).start()

                    @pl.when(owner != me)
                    def _():
                        pltpu.make_async_remote_copy(src, dst, s_send.at[slot, half], s_recv.at[m, chip], **to(owner)).start()

    def sent(p):
        slot = lax.rem(p, 2)
        t = _xor(chip, _mask(core, p))
        for half in range(2):
            @pl.when(2 * t + half != me)
            def _():
                src, dst = place(0, chip, half, slot)
                pltpu.make_async_remote_copy(src, dst, s_send.at[slot, half], s_recv.at[0, chip], **to(partner)).wait_send()

            @pl.when(2 * t + half == me)
            def _():
                for m in range(3):
                    @pl.when((p >= 4 * m) & (p < 4 * m + 4))
                    def _():
                        src, dst = place(m, chip, half, slot)
                        pltpu.make_async_copy(src, dst, s_recv.at[m, chip]).wait()

    def group(p, _):
        slot = lax.rem(p, 2)
        for kc in range(KB):
            i = p * KB + kc
            d = jnp.dot(a_s[:, kc * BLK : (kc + 1) * BLK], arrived(i), preferred_element_type=jnp.float32)
            if kc:
                acc[0] = acc[0] + d
            else:
                acc[0] = d
            fetch(i + RING)
            if kc == 0:
                @pl.when(p > 0)
                def _():
                    send(p - 1)

        @pl.when(p > 1)
        def _():
            sent(p - 2)

        @pl.when(p < 8)
        def _():
            for h in range(2 * HEADS):
                cols = slice(h * HEAD, (h + 1) * HEAD)
                t = acc[0, :, cols].astype(jnp.bfloat16).astype(jnp.float32)
                stage[slot, :, cols] = (t * cos_ref[...] + pltpu.roll(t, HEAD // 2, 1) * sin_ref[...]).astype(jnp.bfloat16)

        @pl.when(p >= 8)
        def _():
            for h in range(2 * HEADS):
                cols = slice(h * HEAD, (h + 1) * HEAD)
                vstage[slot, cols, :] = acc[0, :, cols].T.astype(jnp.bfloat16)

    lax.fori_loop(0, GROUPS, group, None)
    send(jnp.int32(GROUPS - 1))
    for r in range(OWN // LAG):
        a_copy(r).wait_send()

    def received(c, _):
        for m in range(3):
            @pl.when((c != chip) | (lax.rem(core + m, 2) == 1))
            def _():
                src, dst = place(m, c, 0, 0)
                pltpu.make_async_remote_copy(src, dst, s_send.at[0, 0], s_recv.at[m, c], **to(partner)).wait_recv()

    sent(jnp.int32(GROUPS - 2))
    sent(jnp.int32(GROUPS - 1))
    lax.fori_loop(0, CHIPS, received, None)

    def o_copy(iq):
        rows = pl.ds(pl.multiple_of(iq * TOK, TOK), TOK)
        return pltpu.make_async_remote_copy(q_s.at[rows, :], seen.at[chip], o_send.at[iq], o_recv.at[chip], **to(2 * iq + core))

    def own_copy():
        rows = pl.ds(pl.multiple_of(chip * TOK, TOK), TOK)
        return pltpu.make_async_copy(q_s.at[rows, :], seen.at[chip], o_send.at[chip])

    def queries(k, _):
        iq = _xor(chip, _pick(ORDER, k))
        attend_block(q_s, k_s, vt_s, top_s, mix_s, iq)

        @pl.when(iq != chip)
        def _():
            o_copy(iq).start()

        @pl.when(iq == chip)
        def _():
            own_copy().start()

    lax.fori_loop(0, CHIPS, queries, None)

    def p_copy(n):
        slot = lax.rem(n, 2)
        rows = pl.ds(pl.multiple_of((1 - core) * OWN, OWN), OWN)
        return pltpu.make_async_remote_copy(acc.at[slot, rows, :], other.at[slot], p_send.at[slot], p_recv.at[n], **to(partner))

    def y_copy(n):
        cols = pl.ds(pl.multiple_of(n * BLK, BLK), BLK)
        return pltpu.make_async_copy(stage.at[lax.rem(n, 2), :OWN, :], y_ref.at[:, cols], y_sem.at[lax.rem(n, 2)])

    def finish(n):
        slot = lax.rem(n, 2)
        cols = pl.ds(pl.multiple_of(n * BLK, BLK), BLK)
        p_copy(n).wait_recv()

        @pl.when(n > 1)
        def _():
            y_copy(n - 2).wait()

        mine = acc[slot, pl.ds(pl.multiple_of(core * OWN, OWN), OWN), :]
        stage[slot, :OWN, :] = (xbuf[:, cols].astype(jnp.float32) + (mine + other[slot])).astype(jnp.bfloat16)
        y_copy(n).start()

    def out_group(n, _):
        slot = lax.rem(n, 2)
        for b in range(4):
            i = GROUPS * KB + n * 4 + b
            parts = []
            for half in range(2):
                k = 2 * b + half
                c = _xor(chip, ORDER[k])

                @pl.when(n == 0)
                def _():
                    if ORDER[k]:
                        pltpu.make_async_remote_copy(seen.at[c], seen.at[c], o_send.at[c], o_recv.at[c], **to(partner)).wait_recv()
                    else:
                        own_copy().wait()

                parts.append(seen[c])
            if b == 0:
                @pl.when(n > 1)
                def _():
                    p_copy(n - 2).wait_send()

            d = jnp.dot(jnp.concatenate(parts, axis=1), arrived(i), preferred_element_type=jnp.float32)
            if b:
                acc[slot] = acc[slot] + d
            else:
                acc[slot] = d
            fetch(i + RING)
            if b == 1:
                @pl.when(n > 0)
                def _():
                    finish(n - 1)
        p_copy(n).start()

    lax.fori_loop(0, OUTS, out_group, None)
    finish(jnp.int32(OUTS - 1))
    for n in (OUTS - 2, OUTS - 1):
        p_copy(jnp.int32(n)).wait_send()
        y_copy(jnp.int32(n)).wait()

    def drain(c, _):
        @pl.when(c != chip)
        def _():
            o_copy(c).wait_send()

    lax.fori_loop(0, CHIPS, drain, None)


def solution(mesh):
    def step(x, gain, wq, wk, wv, wo):
        me = lax.axis_index("sp")
        place = lax.div(me, 2) * TOK + jnp.arange(TOK)
        half = HEAD // 2
        angle = place.astype(jnp.float32)[:, None] * THETA ** (-jnp.arange(half, dtype=jnp.float32) / half)
        cos, sin = jnp.cos(angle), jnp.sin(angle)
        vmem, hbm = pl.BlockSpec(memory_space=pltpu.VMEM), pl.BlockSpec(memory_space=pl.ANY)
        return pl.pallas_call(
            layer,
            out_shape=jax.ShapeDtypeStruct((OWN, D), jnp.bfloat16),
            in_specs=[hbm, vmem, vmem, vmem, hbm, hbm, hbm, hbm],
            out_specs=hbm,
            scratch_shapes=[
                pltpu.VMEM((TOK, D), jnp.bfloat16),
                pltpu.VMEM((SEQ, W), jnp.bfloat16),
                pltpu.VMEM((SEQ, W), jnp.bfloat16),
                pltpu.VMEM((W, SEQ), jnp.bfloat16),
                pltpu.VMEM((RING, BLK, BLK), jnp.bfloat16),
                pltpu.VMEM((2, TOK, BLK), jnp.float32),
                pltpu.VMEM((2, TOK, BLK), jnp.bfloat16),
                pltpu.VMEM((2, BLK, TOK), jnp.bfloat16),
                pltpu.VMEM((CHIPS, TOK, W), jnp.bfloat16),
                pltpu.VMEM((2, OWN, BLK), jnp.float32),
                pltpu.VMEM((OWN, D), jnp.bfloat16),
                pltpu.VMEM((8, TOK), jnp.float32),
                pltpu.VMEM((HEADS, HEAD + 8, TOK), jnp.float32),
                pltpu.SemaphoreType.DMA((RING,)),
                pltpu.SemaphoreType.DMA,
                pltpu.SemaphoreType.DMA((OWN // LAG,)),
                pltpu.SemaphoreType.DMA((OWN // LAG,)),
                pltpu.SemaphoreType.DMA((2, 2)),
                pltpu.SemaphoreType.DMA((3, CHIPS)),
                pltpu.SemaphoreType.DMA((CHIPS,)),
                pltpu.SemaphoreType.DMA((CHIPS,)),
                pltpu.SemaphoreType.DMA((2,)),
                pltpu.SemaphoreType.DMA((OUTS,)),
                pltpu.SemaphoreType.DMA((2,)),
            ],
            compiler_params=pltpu.CompilerParams(collective_id=0, has_side_effects=True, vmem_limit_bytes=67043328),
            cost_estimate=pl.CostEstimate(flops=160 * 10**9, bytes_accessed=61 * 10**7, transcendentals=15 * 10**6),
        )(x, gain[None, :], jnp.concatenate([cos, cos], 1), jnp.concatenate([-sin, sin], 1), wq, wk, wv, wo)

    tokens, whole = P(("dp", "sp"), None), P(None, None)
    return jax.shard_map(
        step,
        mesh=mesh,
        in_specs=(tokens, P(None), whole, whole, whole, whole),
        out_specs=tokens,
        check_vma=False,
    )
```

```python
import functools

import jax
import jax.numpy as jnp
from jax import lax
from jax.experimental import pallas as pl
from jax.experimental.pallas import tpu as pltpu
from jax.sharding import PartitionSpec as P


HEAD = 128
THETA = 10000
NEG = -1e30
HIDDEN = 2 * NEG
LOG2E = 1.4426950408889634

D = 12288
OWN = 128
TOK = 256
SEQ = 2048
CHIPS = 8
HEADS = 6
W = HEADS * HEAD
BLK = 2 * W
KB = D // BLK
GROUPS = 12
OUTS = D // BLK
RING = 5
BLOCKS = GROUPS * KB + OUTS * 4
VMEM = 60 * 2**20
LAG = 32

ORDER = (7, 3, 4, 5, 2, 6, 1, 0)
TERMS = (7, 3, 4, 0, 5, 2, 6, 1)
SLOTS = OUTS // 2


def _xor(a, b):
    out = 0
    for bit in (1, 2, 4):
        p, q = lax.rem(lax.div(a, bit), 2), lax.rem(lax.div(b, bit), 2)
        out = out + bit * (p + q - 2 * p * q)
    return out


def _mask(core, p):
    m, j = lax.div(p, 4), lax.rem(p, 4)
    jj = 3 - j
    even = 6 - lax.div(jj * (jj + 1), 2)
    odd = lax.rem(core + m, 2)
    return even + odd * (7 - 2 * even)


def _pick(table, k):
    out = 0
    for i, v in enumerate(table):
        out = out + jnp.where(k == i, v, 0)
    return out


def _dot(a, b, ca, cb):
    return lax.dot_general(a, b, (((ca,), (cb,)), ((), ())), preferred_element_type=jnp.float32)


def attend_block(q_ref, k_ref, vt_ref, top_s, mix_s, iq):
    e = HEAD**-0.5 * LOG2E
    rows = pl.ds(pl.multiple_of(iq * TOK, TOK), TOK)
    top_s[...] = jnp.full(top_s.shape, NEG, jnp.float32)
    mix_s[...] = jnp.zeros(mix_s.shape, jnp.float32)

    def block(start, size, masked):
        here = pl.ds(pl.multiple_of(start, TOK), size)
        ones = jnp.ones((8, size), jnp.bfloat16)
        scores = [_dot(k_ref[here, h * HEAD : (h + 1) * HEAD], q_ref[rows, h * HEAD : (h + 1) * HEAD], 1, 1) for h in range(HEADS)]
        if masked:
            ok = lax.broadcasted_iota(jnp.int32, (size, TOK), 0) <= lax.broadcasted_iota(jnp.int32, (size, TOK), 1)
        weights, keeps = [], []
        for h, s in enumerate(scores):
            if masked:
                s = jnp.where(ok, s, HIDDEN)
            old = top_s[h : h + 1, :]
            top = jnp.maximum(old, s.max(axis=0, keepdims=True))
            top_s[h : h + 1, :] = top
            weights.append(jnp.exp2((s - top) * e).astype(jnp.bfloat16))
            keeps.append(jnp.exp2((old - top) * e))
        for h, (p, keep) in enumerate(zip(weights, keeps)):
            values = jnp.concatenate([vt_ref[h * HEAD : (h + 1) * HEAD, here], ones], axis=0)
            mix_s[h] = mix_s[h] * keep + _dot(values, p, 1, 0)

    lax.fori_loop(0, lax.div(iq, 2), lambda j, _: block(j * 2 * TOK, 2 * TOK, False), None)

    @pl.when(lax.rem(iq, 2) == 1)
    def _():
        block((iq - 1) * TOK, TOK, False)

    block(iq * TOK, TOK, True)
    for h in range(HEADS):
        q_ref[rows, h * HEAD : (h + 1) * HEAD] = (mix_s[h, :HEAD, :] * (1 / mix_s[h, HEAD : HEAD + 1, :])).T.astype(jnp.bfloat16)


def layer(x_ref, gain_ref, cos_ref, sin_ref, wq_ref, wk_ref, wv_ref, wo_ref, y_ref,
          a_s, q_s, k_s, vt_s, wbuf, acc, stage, vstage, seen, other, turn, top_s, mix_s,
          w_sem, x_sem, a_send, a_recv, s_send, s_recv, o_send, o_recv, p_send, p_recv):
    me = lax.axis_index("sp")
    chip, core = lax.div(me, 2), lax.rem(me, 2)
    partner = me + 1 - 2 * core

    def to(d):
        return dict(device_id={"sp": d}, device_id_type=pl.DeviceIdType.MESH)

    def slot_of(i):
        return lax.rem(i, RING)

    def source(k):
        return _xor(chip, _pick(TERMS, k))

    def fetch(i):
        slot = slot_of(i)

        def column(w_ref, p):
            cols = pl.ds(pl.multiple_of(_xor(chip, _mask(core, p)) * BLK, BLK), BLK)
            rows = pl.ds(pl.multiple_of(lax.rem(i, KB) * BLK, BLK), BLK)
            pltpu.make_async_copy(w_ref.at[rows, cols], wbuf.at[slot], w_sem.at[slot]).start()

        p = lax.div(i, KB)
        for m, w_ref in enumerate((wk_ref, wv_ref, wq_ref)):
            @pl.when((p >= 4 * m) & (p < 4 * m + 4))
            def _():
                column(w_ref, p)

        @pl.when((i >= GROUPS * KB) & (i < BLOCKS))
        def _():
            j = i - GROUPS * KB
            late = lax.div(j, 2 * SLOTS)
            n = jnp.where(late > 1, lax.div(j, 4), lax.div(lax.rem(j, 2 * SLOTS), 2))
            b = jnp.where(late > 1, lax.rem(j, 4), 2 * late + lax.rem(j, 2))
            cols = pl.ds(pl.multiple_of(n * BLK, BLK), BLK)
            for half in range(2):
                rows = pl.ds(pl.multiple_of((2 * source(2 * b + half) + core) * W, W), W)
                pltpu.make_async_copy(wo_ref.at[rows, cols], wbuf.at[slot, half * W : (half + 1) * W, :], w_sem.at[slot]).start()

    def arrived(i):
        slot = slot_of(i)
        pltpu.make_async_copy(wq_ref.at[:BLK, :BLK], wbuf.at[slot], w_sem.at[slot]).wait()
        return wbuf[slot]

    x_in = pltpu.make_async_copy(x_ref, y_ref, x_sem)
    x_in.start()
    for i in range(RING):
        fetch(jnp.int32(i))

    barrier = pltpu.get_barrier_semaphore()
    for step in range(1, 16):
        pl.semaphore_signal(barrier, inc=1, **to(lax.rem(me + step, 16)))
    pl.semaphore_wait(barrier, 15)

    turn[0] = jnp.concatenate([cos_ref[...], cos_ref[...]], axis=1)
    turn[1] = jnp.concatenate([-sin_ref[...], sin_ref[...]], axis=1)
    gain = gain_ref[...].astype(jnp.float32)[None, :]

    x_in.wait()

    def a_copy(r):
        rows = pl.ds(pl.multiple_of(core * OWN + r * LAG, LAG), LAG)
        return pltpu.make_async_remote_copy(a_s.at[rows, :], a_s.at[rows, :], a_send.at[r], a_recv.at[r], **to(partner))

    for r in range(OWN // LAG):
        wide = y_ref[r * LAG : (r + 1) * LAG, :].astype(jnp.float32)
        scale = lax.rsqrt(jnp.mean(wide * wide, -1, keepdims=True) + 1e-6)
        rows = pl.ds(pl.multiple_of(core * OWN + r * LAG, LAG), LAG)
        a_s[rows, :] = (wide * scale * gain).astype(jnp.bfloat16)
        if r:
            a_copy(r - 1).start()
    a_copy(OWN // LAG - 1).start()
    for r in range(OWN // LAG):
        rows = pl.ds(pl.multiple_of((1 - core) * OWN + r * LAG, LAG), LAG)
        pltpu.make_async_remote_copy(a_s.at[rows, :], a_s.at[rows, :], a_send.at[r], a_recv.at[r], **to(partner)).wait_recv()

    def place(m, ref, half, slot):
        if m == 1:
            return vstage.at[slot, half * W : (half + 1) * W, :], vt_s.at[:, pl.ds(pl.multiple_of(ref * TOK, TOK), TOK)]
        return (stage.at[slot, :, half * W : (half + 1) * W], (k_s, None, q_s)[m].at[pl.ds(pl.multiple_of(ref * TOK, TOK), TOK), :])

    def send(p):
        slot = lax.rem(p, 2)
        t = _xor(chip, _mask(core, p))
        for m in range(3):
            @pl.when((p >= 4 * m) & (p < 4 * m + 4))
            def _():
                for half in range(2):
                    src, dst = place(m, chip, half, slot)
                    owner = 2 * t + half

                    @pl.when(owner == me)
                    def _():
                        pltpu.make_async_copy(src, dst, s_recv.at[m, chip]).start()

                    @pl.when(owner != me)
                    def _():
                        pltpu.make_async_remote_copy(src, dst, s_send.at[slot, half], s_recv.at[m, chip], **to(owner)).start()

    def sent(p):
        slot = lax.rem(p, 2)
        t = _xor(chip, _mask(core, p))
        for half in range(2):
            @pl.when(2 * t + half != me)
            def _():
                src, dst = place(0, chip, half, slot)
                pltpu.make_async_remote_copy(src, dst, s_send.at[slot, half], s_recv.at[0, chip], **to(partner)).wait_send()

            @pl.when(2 * t + half == me)
            def _():
                for m in range(3):
                    @pl.when((p >= 4 * m) & (p < 4 * m + 4))
                    def _():
                        src, dst = place(m, chip, half, slot)
                        pltpu.make_async_copy(src, dst, s_recv.at[m, chip]).wait()

    def group(p, _):
        slot = lax.rem(p, 2)
        for kc in range(KB):
            i = p * KB + kc
            d = jnp.dot(a_s[:, kc * BLK : (kc + 1) * BLK], arrived(i), preferred_element_type=jnp.float32)
            if kc:
                acc[0] = acc[0] + d
            else:
                acc[0] = d
            fetch(i + RING)
            if kc == 0:
                @pl.when(p > 0)
                def _():
                    send(p - 1)

        @pl.when(p > 1)
        def _():
            sent(p - 2)

        @pl.when(lax.div(p, 4) != 1)
        def _():
            for h in range(2 * HEADS):
                cols = slice(h * HEAD, (h + 1) * HEAD)
                t = acc[0, :, cols].astype(jnp.bfloat16).astype(jnp.float32)
                stage[slot, :, cols] = (t * turn[0] + pltpu.roll(t, HEAD // 2, 1) * turn[1]).astype(jnp.bfloat16)

        @pl.when(lax.div(p, 4) == 1)
        def _():
            for h in range(2 * HEADS):
                cols = slice(h * HEAD, (h + 1) * HEAD)
                vstage[slot, cols, :] = acc[0, :, cols].T.astype(jnp.bfloat16)

    lax.fori_loop(0, GROUPS, group, None)
    send(jnp.int32(GROUPS - 1))
    for r in range(OWN // LAG):
        a_copy(r).wait_send()

    def received(m, c):
        @pl.when((c != chip) | (lax.rem(core + m, 2) == 1))
        def _():
            src, dst = place(m, c, 0, 0)
            pltpu.make_async_remote_copy(src, dst, s_send.at[0, 0], s_recv.at[m, c], **to(partner)).wait_recv()

    def keys_and_values(c, _):
        received(0, c)
        received(1, c)

    lax.fori_loop(0, CHIPS, keys_and_values, None)

    def o_copy(iq):
        rows = pl.ds(pl.multiple_of(iq * TOK, TOK), TOK)
        return pltpu.make_async_remote_copy(q_s.at[rows, :], seen.at[chip], o_send.at[iq], o_recv.at[chip], **to(2 * iq + core))

    def own_copy():
        rows = pl.ds(pl.multiple_of(chip * TOK, TOK), TOK)
        return pltpu.make_async_copy(q_s.at[rows, :], seen.at[chip], o_send.at[chip])

    def queries(k, _):
        iq = _xor(chip, _pick(ORDER, k))
        received(2, iq)
        attend_block(q_s, k_s, vt_s, top_s, mix_s, iq)

        @pl.when(iq != chip)
        def _():
            o_copy(iq).start()

        @pl.when(iq == chip)
        def _():
            own_copy().start()

    lax.fori_loop(0, CHIPS, queries, None)

    sent(jnp.int32(GROUPS - 2))
    sent(jnp.int32(GROUPS - 1))

    def p_copy(n):
        slot = lax.rem(n, SLOTS)
        rows = pl.ds(pl.multiple_of((1 - core) * OWN, OWN), OWN)
        return pltpu.make_async_remote_copy(acc.at[slot, rows, :], other.at[lax.rem(n, 2)], p_send.at[slot], p_recv.at[n], **to(partner))

    def finish(n):
        cols = pl.ds(pl.multiple_of(n * BLK, BLK), BLK)
        p_copy(n).wait_recv()
        mine = acc[lax.rem(n, SLOTS), pl.ds(pl.multiple_of(core * OWN, OWN), OWN), :]
        y_ref[:, cols] = (y_ref[:, cols].astype(jnp.float32) + (mine + other[lax.rem(n, 2)])).astype(jnp.bfloat16)

    def arrival(k):
        c = _xor(chip, TERMS[k])
        if TERMS[k]:
            pltpu.make_async_remote_copy(seen.at[c], seen.at[c], o_send.at[c], o_recv.at[c], **to(partner)).wait_recv()
        else:
            own_copy().wait()

    def add(i, slot, b):
        terms = jnp.concatenate([seen[_xor(chip, TERMS[2 * b])], seen[_xor(chip, TERMS[2 * b + 1])]], axis=1)
        d = jnp.dot(terms, arrived(i), preferred_element_type=jnp.float32)
        if b:
            acc[slot] = acc[slot] + d
        else:
            acc[slot] = d
        fetch(i + RING)

    def last_group(n):
        @pl.when(n > 0)
        def _():
            finish(n - 1)

    first = GROUPS * KB
    for k in range(4):
        arrival(k)

    def early(n, _):
        add(first + 2 * n, n, 0)
        add(first + 2 * n + 1, n, 1)

    lax.fori_loop(0, SLOTS, early, None)
    for k in range(4, 8):
        arrival(k)

    def late(n, _):
        add(first + 2 * (SLOTS + n), n, 2)
        last_group(n)
        add(first + 2 * (SLOTS + n) + 1, n, 3)
        p_copy(n).start()

    lax.fori_loop(0, SLOTS, late, None)

    def whole(n, _):
        slot = lax.rem(n, SLOTS)
        p_copy(n - SLOTS).wait_send()
        for b in range(4):
            add(first + 4 * n + b, slot, b)
            if b == 1:
                last_group(n)
        p_copy(n).start()

    lax.fori_loop(SLOTS, OUTS, whole, None)
    finish(jnp.int32(OUTS - 1))
    for n in range(OUTS - SLOTS, OUTS):
        p_copy(jnp.int32(n)).wait_send()

    def drain(c, _):
        @pl.when(c != chip)
        def _():
            o_copy(c).wait_send()

    lax.fori_loop(0, CHIPS, drain, None)


def solution(mesh):
    def step(x, gain, wq, wk, wv, wo):
        me = lax.axis_index("sp")
        place = lax.div(me, 2) * TOK + jnp.arange(TOK)
        half = HEAD // 2
        angle = place.astype(jnp.float32)[:, None] * THETA ** (-jnp.arange(half, dtype=jnp.float32) / half)
        cos, sin = jnp.cos(angle), jnp.sin(angle)
        vmem, hbm = pl.BlockSpec(memory_space=pltpu.VMEM), pl.BlockSpec(memory_space=pl.ANY)
        return pl.pallas_call(
            layer,
            out_shape=pltpu.VMEM((OWN, D), jnp.bfloat16),
            in_specs=[hbm, vmem, vmem, vmem, hbm, hbm, hbm, hbm],
            out_specs=vmem,
            scratch_shapes=[
                pltpu.VMEM((TOK, D), jnp.bfloat16),
                pltpu.VMEM((SEQ, W), jnp.bfloat16),
                pltpu.VMEM((SEQ, W), jnp.bfloat16),
                pltpu.VMEM((W, SEQ), jnp.bfloat16),
                pltpu.VMEM((RING, BLK, BLK), jnp.bfloat16),
                pltpu.VMEM((SLOTS, TOK, BLK), jnp.float32),
                pltpu.VMEM((2, TOK, BLK), jnp.bfloat16),
                pltpu.VMEM((2, BLK, TOK), jnp.bfloat16),
                pltpu.VMEM((CHIPS, TOK, W), jnp.bfloat16),
                pltpu.VMEM((2, OWN, BLK), jnp.float32),
                pltpu.VMEM((2, TOK, HEAD), jnp.float32),
                pltpu.VMEM((8, TOK), jnp.float32),
                pltpu.VMEM((HEADS, HEAD + 8, TOK), jnp.float32),
                pltpu.SemaphoreType.DMA((RING,)),
                pltpu.SemaphoreType.DMA,
                pltpu.SemaphoreType.DMA((OWN // LAG,)),
                pltpu.SemaphoreType.DMA((OWN // LAG,)),
                pltpu.SemaphoreType.DMA((2, 2)),
                pltpu.SemaphoreType.DMA((3, CHIPS)),
                pltpu.SemaphoreType.DMA((CHIPS,)),
                pltpu.SemaphoreType.DMA((CHIPS,)),
                pltpu.SemaphoreType.DMA((SLOTS,)),
                pltpu.SemaphoreType.DMA((OUTS,)),
            ],
            compiler_params=pltpu.CompilerParams(collective_id=0, has_side_effects=True, vmem_limit_bytes=VMEM),
            cost_estimate=pl.CostEstimate(flops=160 * 10**9, bytes_accessed=61 * 10**7, transcendentals=15 * 10**6),
        )(x, gain, cos, sin, wq, wk, wv, wo)

    tokens, whole = P(("dp", "sp"), None), P(None, None)
    return jax.shard_map(
        step,
        mesh=mesh,
        in_specs=(tokens, P(None), whole, whole, whole, whole),
        out_specs=tokens,
        check_vma=False,
    )
```

```python
import functools

import jax
import jax.numpy as jnp
from jax import lax
from jax.experimental import pallas as pl
from jax.experimental.pallas import tpu as pltpu
from jax.sharding import PartitionSpec as P


HEAD = 128
THETA = 10000
NEG = -1e30
HIDDEN = 2 * NEG
LOG2E = 1.4426950408889634

D = 12288
OWN = 128
TOK = 256
SEQ = 2048
CHIPS = 8
HEADS = 6
W = HEADS * HEAD
BLK = 2 * W
KB = D // BLK
GROUPS = 12
OUTS = D // BLK
RING = 4
BLOCKS = GROUPS * KB + OUTS * 4
VMEM = 67043328 - 3 * 2**20 - 2**17
LAG = 32

ORDER = (7, 3, 4, 5, 2, 6, 1, 0)
TERMS = (7, 3, 4, 0, 5, 2, 6, 1)


def _xor(a, b):
    out = 0
    for bit in (1, 2, 4):
        p, q = lax.rem(lax.div(a, bit), 2), lax.rem(lax.div(b, bit), 2)
        out = out + bit * (p + q - 2 * p * q)
    return out


def _mask(core, p):
    m, j = lax.div(p, 4), lax.rem(p, 4)
    jj = 3 - j
    even = 6 - lax.div(jj * (jj + 1), 2)
    odd = lax.rem(core + m, 2)
    return even + odd * (7 - 2 * even)


def _pick(table, k):
    out = 0
    for i, v in enumerate(table):
        out = out + jnp.where(k == i, v, 0)
    return out


def _dot(a, b, ca, cb):
    return lax.dot_general(a, b, (((ca,), (cb,)), ((), ())), preferred_element_type=jnp.float32)


def attend_block(q_ref, k_ref, vt_ref, top_s, mix_s, iq):
    e = HEAD**-0.5 * LOG2E
    rows = pl.ds(pl.multiple_of(iq * TOK, TOK), TOK)
    top_s[...] = jnp.full(top_s.shape, NEG, jnp.float32)
    mix_s[...] = jnp.zeros(mix_s.shape, jnp.float32)

    def block(start, size, masked):
        here = pl.ds(pl.multiple_of(start, TOK), size)
        ones = jnp.ones((8, size), jnp.bfloat16)
        scores = [_dot(k_ref[here, h * HEAD : (h + 1) * HEAD], q_ref[rows, h * HEAD : (h + 1) * HEAD], 1, 1) for h in range(HEADS)]
        if masked:
            ok = lax.broadcasted_iota(jnp.int32, (size, TOK), 0) <= lax.broadcasted_iota(jnp.int32, (size, TOK), 1)
        weights, keeps = [], []
        for h, s in enumerate(scores):
            if masked:
                s = jnp.where(ok, s, HIDDEN)
            old = top_s[h : h + 1, :]
            top = jnp.maximum(old, s.max(axis=0, keepdims=True))
            top_s[h : h + 1, :] = top
            weights.append(jnp.exp2((s - top) * e).astype(jnp.bfloat16))
            keeps.append(jnp.exp2((old - top) * e))
        for h, (p, keep) in enumerate(zip(weights, keeps)):
            values = jnp.concatenate([vt_ref[h * HEAD : (h + 1) * HEAD, here], ones], axis=0)
            mix_s[h] = mix_s[h] * keep + _dot(values, p, 1, 0)

    lax.fori_loop(0, lax.div(iq, 2), lambda j, _: block(j * 2 * TOK, 2 * TOK, False), None)

    @pl.when(lax.rem(iq, 2) == 1)
    def _():
        block((iq - 1) * TOK, TOK, False)

    block(iq * TOK, TOK, True)
    for h in range(HEADS):
        q_ref[rows, h * HEAD : (h + 1) * HEAD] = (mix_s[h, :HEAD, :] * (1 / mix_s[h, HEAD : HEAD + 1, :])).T.astype(jnp.bfloat16)


def layer(x_ref, gain_ref, cos_ref, sin_ref, wq_ref, wk_ref, wv_ref, wo_ref, y_ref,
          a_s, q_s, k_s, vt_s, wbuf, acc, stage, vstage, seen, other, turn, top_s, mix_s,
          w_sem, x_sem, a_send, a_recv, s_send, s_recv, o_send, o_recv, p_send, p_recv):
    me = lax.axis_index("sp")
    chip, core = lax.div(me, 2), lax.rem(me, 2)
    partner = me + 1 - 2 * core

    def to(d):
        return dict(device_id={"sp": d}, device_id_type=pl.DeviceIdType.MESH)

    def slot_of(i):
        return lax.rem(i, RING)

    def source(k):
        return _xor(chip, _pick(TERMS, k))

    def fetch(i):
        slot = slot_of(i)

        def column(w_ref, p):
            cols = pl.ds(pl.multiple_of(_xor(chip, _mask(core, p)) * BLK, BLK), BLK)
            rows = pl.ds(pl.multiple_of(lax.rem(i, KB) * BLK, BLK), BLK)
            pltpu.make_async_copy(w_ref.at[rows, cols], wbuf.at[slot], w_sem.at[slot]).start()

        p = lax.div(i, KB)
        for m, w_ref in enumerate((wk_ref, wv_ref, wq_ref)):
            @pl.when((p >= 4 * m) & (p < 4 * m + 4))
            def _():
                column(w_ref, p)

        @pl.when((i >= GROUPS * KB) & (i < BLOCKS))
        def _():
            j = i - GROUPS * KB
            ends = j >= 2 * OUTS
            n = jnp.where(ends, lax.div(j, 2) - OUTS, lax.rem(j, OUTS))
            b = jnp.where(ends, 2 + lax.rem(j, 2), lax.div(j, OUTS))
            cols = pl.ds(pl.multiple_of(n * BLK, BLK), BLK)
            for half in range(2):
                rows = pl.ds(pl.multiple_of((2 * source(2 * b + half) + core) * W, W), W)
                pltpu.make_async_copy(wo_ref.at[rows, cols], wbuf.at[slot, half * W : (half + 1) * W, :], w_sem.at[slot]).start()

    def arrived(i):
        slot = slot_of(i)
        pltpu.make_async_copy(wq_ref.at[:BLK, :BLK], wbuf.at[slot], w_sem.at[slot]).wait()
        return wbuf[slot]

    x_in = pltpu.make_async_copy(x_ref, y_ref, x_sem)
    x_in.start()
    for i in range(RING):
        fetch(jnp.int32(i))

    barrier = pltpu.get_barrier_semaphore()
    for step in range(1, 16):
        pl.semaphore_signal(barrier, inc=1, **to(lax.rem(me + step, 16)))

    turn[0] = jnp.concatenate([cos_ref[...], cos_ref[...]], axis=1)
    turn[1] = jnp.concatenate([-sin_ref[...], sin_ref[...]], axis=1)
    gain = gain_ref[...].astype(jnp.float32)[None, :]

    x_in.wait()

    def a_copy(r):
        rows = pl.ds(pl.multiple_of(core * OWN + r * LAG, LAG), LAG)
        return pltpu.make_async_remote_copy(a_s.at[rows, :], a_s.at[rows, :], a_send.at[r], a_recv.at[r], **to(partner))

    for r in range(OWN // LAG):
        wide = y_ref[r * LAG : (r + 1) * LAG, :].astype(jnp.float32)
        scale = lax.rsqrt(jnp.mean(wide * wide, -1, keepdims=True) + 1e-6)
        rows = pl.ds(pl.multiple_of(core * OWN + r * LAG, LAG), LAG)
        a_s[rows, :] = (wide * scale * gain).astype(jnp.bfloat16)
        if r == 0:
            pl.semaphore_wait(barrier, 15)
        else:
            a_copy(r - 1).start()
    a_copy(OWN // LAG - 1).start()
    for r in range(OWN // LAG):
        rows = pl.ds(pl.multiple_of((1 - core) * OWN + r * LAG, LAG), LAG)
        pltpu.make_async_remote_copy(a_s.at[rows, :], a_s.at[rows, :], a_send.at[r], a_recv.at[r], **to(partner)).wait_recv()

    def place(m, ref, half, slot):
        if m == 1:
            return vstage.at[slot, half * W : (half + 1) * W, :], vt_s.at[:, pl.ds(pl.multiple_of(ref * TOK, TOK), TOK)]
        return (stage.at[slot, :, half * W : (half + 1) * W], (k_s, None, q_s)[m].at[pl.ds(pl.multiple_of(ref * TOK, TOK), TOK), :])

    def send(p):
        slot = lax.rem(p, 2)
        t = _xor(chip, _mask(core, p))
        for m in range(3):
            @pl.when((p >= 4 * m) & (p < 4 * m + 4))
            def _():
                for half in range(2):
                    src, dst = place(m, chip, half, slot)
                    owner = 2 * t + half

                    @pl.when(owner == me)
                    def _():
                        pltpu.make_async_copy(src, dst, s_recv.at[m, chip]).start()

                    @pl.when(owner != me)
                    def _():
                        pltpu.make_async_remote_copy(src, dst, s_send.at[slot, half], s_recv.at[m, chip], **to(owner)).start()

    def sent(p):
        slot = lax.rem(p, 2)
        t = _xor(chip, _mask(core, p))
        for half in range(2):
            @pl.when(2 * t + half != me)
            def _():
                src, dst = place(0, chip, half, slot)
                pltpu.make_async_remote_copy(src, dst, s_send.at[slot, half], s_recv.at[0, chip], **to(partner)).wait_send()

            @pl.when(2 * t + half == me)
            def _():
                for m in range(3):
                    @pl.when((p >= 4 * m) & (p < 4 * m + 4))
                    def _():
                        src, dst = place(m, chip, half, slot)
                        pltpu.make_async_copy(src, dst, s_recv.at[m, chip]).wait()

    def group(p, _):
        slot = lax.rem(p, 2)
        for kc in range(KB):
            i = p * KB + kc
            d = jnp.dot(a_s[:, kc * BLK : (kc + 1) * BLK], arrived(i), preferred_element_type=jnp.float32)
            if kc:
                acc[0] = acc[0] + d
            else:
                acc[0] = d
            fetch(i + RING)
            if kc == 0:
                @pl.when(p > 0)
                def _():
                    send(p - 1)

        @pl.when(p > 1)
        def _():
            sent(p - 2)

        @pl.when(lax.div(p, 4) != 1)
        def _():
            for h in range(2 * HEADS):
                cols = slice(h * HEAD, (h + 1) * HEAD)
                t = acc[0, :, cols].astype(jnp.bfloat16).astype(jnp.float32)
                stage[slot, :, cols] = (t * turn[0] + pltpu.roll(t, HEAD // 2, 1) * turn[1]).astype(jnp.bfloat16)

        @pl.when(lax.div(p, 4) == 1)
        def _():
            for h in range(2 * HEADS):
                cols = slice(h * HEAD, (h + 1) * HEAD)
                vstage[slot, cols, :] = acc[0, :, cols].T.astype(jnp.bfloat16)

    lax.fori_loop(0, GROUPS, group, None)
    send(jnp.int32(GROUPS - 1))
    for r in range(OWN // LAG):
        a_copy(r).wait_send()

    def received(m, c):
        @pl.when((c != chip) | (lax.rem(core + m, 2) == 1))
        def _():
            src, dst = place(m, c, 0, 0)
            pltpu.make_async_remote_copy(src, dst, s_send.at[0, 0], s_recv.at[m, c], **to(partner)).wait_recv()

    def keys_and_values(c, _):
        received(0, c)
        received(1, c)

    lax.fori_loop(0, CHIPS, keys_and_values, None)

    def o_copy(iq):
        rows = pl.ds(pl.multiple_of(iq * TOK, TOK), TOK)
        return pltpu.make_async_remote_copy(q_s.at[rows, :], seen.at[chip], o_send.at[iq], o_recv.at[chip], **to(2 * iq + core))

    def own_copy():
        rows = pl.ds(pl.multiple_of(chip * TOK, TOK), TOK)
        return pltpu.make_async_copy(q_s.at[rows, :], seen.at[chip], o_send.at[chip])

    def queries(k, _):
        iq = _xor(chip, _pick(ORDER, k))
        received(2, iq)
        attend_block(q_s, k_s, vt_s, top_s, mix_s, iq)

        @pl.when(iq != chip)
        def _():
            o_copy(iq).start()

        @pl.when(iq == chip)
        def _():
            own_copy().start()

    lax.fori_loop(0, CHIPS, queries, None)

    sent(jnp.int32(GROUPS - 2))
    sent(jnp.int32(GROUPS - 1))

    def p_copy(n):
        rows = pl.ds(pl.multiple_of((1 - core) * OWN, OWN), OWN)
        return pltpu.make_async_remote_copy(acc.at[n, rows, :], other.at[lax.rem(n, 2)], p_send.at[n], p_recv.at[n], **to(partner))

    def finish(n):
        cols = pl.ds(pl.multiple_of(n * BLK, BLK), BLK)
        p_copy(n).wait_recv()
        mine = acc[n, pl.ds(pl.multiple_of(core * OWN, OWN), OWN), :]
        y_ref[:, cols] = (y_ref[:, cols].astype(jnp.float32) + (mine + other[lax.rem(n, 2)])).astype(jnp.bfloat16)

    def arrival(k):
        c = _xor(chip, TERMS[k])
        if TERMS[k]:
            pltpu.make_async_remote_copy(seen.at[c], seen.at[c], o_send.at[c], o_recv.at[c], **to(partner)).wait_recv()
        else:
            own_copy().wait()

    def add(i, n, b):
        terms = jnp.concatenate([seen[_xor(chip, TERMS[2 * b])], seen[_xor(chip, TERMS[2 * b + 1])]], axis=1)
        d = jnp.dot(terms, arrived(i), preferred_element_type=jnp.float32)
        if b:
            acc[n] = acc[n] + d
        else:
            acc[n] = d
        fetch(i + RING)

    first = GROUPS * KB
    for b in range(2):
        arrival(2 * b)
        arrival(2 * b + 1)
        lax.fori_loop(0, OUTS, lambda n, _: add(first + b * OUTS + n, n, b), None)
    for k in range(4, 8):
        arrival(k)

    def ending(n, _):
        add(first + 2 * (OUTS + n), n, 2)

        @pl.when(n > 0)
        def _():
            finish(n - 1)

        add(first + 2 * (OUTS + n) + 1, n, 3)
        p_copy(n).start()

    lax.fori_loop(0, OUTS, ending, None)
    finish(jnp.int32(OUTS - 1))
    for n in range(OUTS):
        p_copy(jnp.int32(n)).wait_send()

    def drain(c, _):
        @pl.when(c != chip)
        def _():
            o_copy(c).wait_send()

    lax.fori_loop(0, CHIPS, drain, None)


def solution(mesh):
    def step(x, gain, wq, wk, wv, wo):
        me = lax.axis_index("sp")
        place = lax.div(me, 2) * TOK + jnp.arange(TOK)
        half = HEAD // 2
        angle = place.astype(jnp.float32)[:, None] * THETA ** (-jnp.arange(half, dtype=jnp.float32) / half)
        cos, sin = jnp.cos(angle), jnp.sin(angle)
        vmem, hbm = pl.BlockSpec(memory_space=pltpu.VMEM), pl.BlockSpec(memory_space=pl.ANY)
        return pl.pallas_call(
            layer,
            out_shape=pltpu.VMEM((OWN, D), jnp.bfloat16),
            in_specs=[hbm, vmem, vmem, vmem, hbm, hbm, hbm, hbm],
            out_specs=vmem,
            scratch_shapes=[
                pltpu.VMEM((TOK, D), jnp.bfloat16),
                pltpu.VMEM((SEQ, W), jnp.bfloat16),
                pltpu.VMEM((SEQ, W), jnp.bfloat16),
                pltpu.VMEM((W, SEQ), jnp.bfloat16),
                pltpu.VMEM((RING, BLK, BLK), jnp.bfloat16),
                pltpu.VMEM((OUTS, TOK, BLK), jnp.float32),
                pltpu.VMEM((2, TOK, BLK), jnp.bfloat16),
                pltpu.VMEM((2, BLK, TOK), jnp.bfloat16),
                pltpu.VMEM((CHIPS, TOK, W), jnp.bfloat16),
                pltpu.VMEM((2, OWN, BLK), jnp.float32),
                pltpu.VMEM((2, TOK, HEAD), jnp.float32),
                pltpu.VMEM((8, TOK), jnp.float32),
                pltpu.VMEM((HEADS, HEAD + 8, TOK), jnp.float32),
                pltpu.SemaphoreType.DMA((RING,)),
                pltpu.SemaphoreType.DMA,
                pltpu.SemaphoreType.DMA((OWN // LAG,)),
                pltpu.SemaphoreType.DMA((OWN // LAG,)),
                pltpu.SemaphoreType.DMA((2, 2)),
                pltpu.SemaphoreType.DMA((3, CHIPS)),
                pltpu.SemaphoreType.DMA((CHIPS,)),
                pltpu.SemaphoreType.DMA((CHIPS,)),
                pltpu.SemaphoreType.DMA((OUTS,)),
                pltpu.SemaphoreType.DMA((OUTS,)),
            ],
            compiler_params=pltpu.CompilerParams(collective_id=0, has_side_effects=True, vmem_limit_bytes=VMEM),
            cost_estimate=pl.CostEstimate(flops=160 * 10**9, bytes_accessed=61 * 10**7, transcendentals=15 * 10**6),
        )(x, gain, cos, sin, wq, wk, wv, wo)

    tokens, whole = P(("dp", "sp"), None), P(None, None)
    return jax.shard_map(
        step,
        mesh=mesh,
        in_specs=(tokens, P(None), whole, whole, whole, whole),
        out_specs=tokens,
        check_vma=False,
    )
```

```python
import functools

import jax
import jax.numpy as jnp
from jax import lax
from jax.experimental import pallas as pl
from jax.experimental.pallas import tpu as pltpu
from jax.sharding import PartitionSpec as P


HEAD = 128
THETA = 10000
NEG = -1e30
HIDDEN = 2 * NEG
LOG2E = 1.4426950408889634

D = 12288
OWN = 128
TOK = 256
SEQ = 2048
CHIPS = 8
HEADS = 6
W = HEADS * HEAD
BLK = 2 * W
KB = D // BLK
GROUPS = 12
OUTS = D // BLK
RING = 4
BLOCKS = GROUPS * KB + OUTS * 4
VMEM = 67043328 - 3 * 2**20 - 2**17
LAG = 32

ORDER = (7, 3, 4, 5, 2, 6, 0, 1)
TERMS = (7, 0, 3, 4, 5, 2, 6, 1)


def _xor(a, b):
    out = 0
    for bit in (1, 2, 4):
        p, q = lax.rem(lax.div(a, bit), 2), lax.rem(lax.div(b, bit), 2)
        out = out + bit * (p + q - 2 * p * q)
    return out


def _mask(core, p):
    m, j = lax.div(p, 4), lax.rem(p, 4)
    jj = 3 - j
    even = 6 - lax.div(jj * (jj + 1), 2)
    odd = lax.rem(core + m, 2)
    return even + odd * (7 - 2 * even)


def _pick(table, k):
    out = 0
    for i, v in enumerate(table):
        out = out + jnp.where(k == i, v, 0)
    return out


def _dot(a, b, ca, cb):
    return lax.dot_general(a, b, (((ca,), (cb,)), ((), ())), preferred_element_type=jnp.float32)


def attend_block(q_ref, k_ref, vt_ref, top_s, mix_s, iq):
    e = HEAD**-0.5 * LOG2E
    rows = pl.ds(pl.multiple_of(iq * TOK, TOK), TOK)
    top_s[...] = jnp.full(top_s.shape, NEG, jnp.float32)
    mix_s[...] = jnp.zeros(mix_s.shape, jnp.float32)

    def block(start, size, masked):
        here = pl.ds(pl.multiple_of(start, TOK), size)
        ones = jnp.ones((8, size), jnp.bfloat16)
        scores = [_dot(k_ref[here, h * HEAD : (h + 1) * HEAD], q_ref[rows, h * HEAD : (h + 1) * HEAD], 1, 1) for h in range(HEADS)]
        if masked:
            ok = lax.broadcasted_iota(jnp.int32, (size, TOK), 0) <= lax.broadcasted_iota(jnp.int32, (size, TOK), 1)
        weights, keeps = [], []
        for h, s in enumerate(scores):
            if masked:
                s = jnp.where(ok, s, HIDDEN)
            old = top_s[h : h + 1, :]
            top = jnp.maximum(old, s.max(axis=0, keepdims=True))
            top_s[h : h + 1, :] = top
            weights.append(jnp.exp2((s - top) * e).astype(jnp.bfloat16))
            keeps.append(jnp.exp2((old - top) * e))
        for h, (p, keep) in enumerate(zip(weights, keeps)):
            values = jnp.concatenate([vt_ref[h * HEAD : (h + 1) * HEAD, here], ones], axis=0)
            mix_s[h] = mix_s[h] * keep + _dot(values, p, 1, 0)

    lax.fori_loop(0, lax.div(iq, 2), lambda j, _: block(j * 2 * TOK, 2 * TOK, False), None)

    @pl.when(lax.rem(iq, 2) == 1)
    def _():
        block((iq - 1) * TOK, TOK, False)

    block(iq * TOK, TOK, True)
    for h in range(HEADS):
        q_ref[rows, h * HEAD : (h + 1) * HEAD] = (mix_s[h, :HEAD, :] * (1 / mix_s[h, HEAD : HEAD + 1, :])).T.astype(jnp.bfloat16)


def layer(x_ref, gain_ref, cos_ref, sin_ref, wq_ref, wk_ref, wv_ref, wo_ref, y_ref,
          a_s, q_s, k_s, vt_s, wbuf, acc, stage, vstage, seen, other, turn, top_s, mix_s,
          w_sem, x_sem, a_send, a_recv, s_send, s_recv, o_send, o_recv, p_send, p_recv):
    me = lax.axis_index("sp")
    chip, core = lax.div(me, 2), lax.rem(me, 2)
    partner = me + 1 - 2 * core

    def to(d):
        return dict(device_id={"sp": d}, device_id_type=pl.DeviceIdType.MESH)

    def slot_of(i):
        return lax.rem(i, RING)

    def source(k):
        return _xor(chip, _pick(TERMS, k))

    def fetch(i):
        slot = slot_of(i)

        def column(w_ref, p):
            cols = pl.ds(pl.multiple_of(_xor(chip, _mask(core, p)) * BLK, BLK), BLK)
            rows = pl.ds(pl.multiple_of(lax.rem(i, KB) * BLK, BLK), BLK)
            pltpu.make_async_copy(w_ref.at[rows, cols], wbuf.at[slot], w_sem.at[slot]).start()

        p = lax.div(i, KB)
        for m, w_ref in enumerate((wk_ref, wv_ref, wq_ref)):
            @pl.when((p >= 4 * m) & (p < 4 * m + 4))
            def _():
                column(w_ref, p)

        @pl.when((i >= GROUPS * KB) & (i < BLOCKS))
        def _():
            j = i - GROUPS * KB
            ends = j >= 2 * OUTS
            n = jnp.where(ends, lax.div(j, 2) - OUTS, lax.rem(j, OUTS))
            b = jnp.where(ends, 2 + lax.rem(j, 2), lax.div(j, OUTS))
            cols = pl.ds(pl.multiple_of(n * BLK, BLK), BLK)
            for half in range(2):
                rows = pl.ds(pl.multiple_of((2 * source(2 * b + half) + core) * W, W), W)
                pltpu.make_async_copy(wo_ref.at[rows, cols], wbuf.at[slot, half * W : (half + 1) * W, :], w_sem.at[slot]).start()

    def arrived(i):
        slot = slot_of(i)
        pltpu.make_async_copy(wq_ref.at[:BLK, :BLK], wbuf.at[slot], w_sem.at[slot]).wait()
        return wbuf[slot]

    x_in = pltpu.make_async_copy(x_ref, y_ref, x_sem)
    x_in.start()
    for i in range(RING):
        fetch(jnp.int32(i))

    barrier = pltpu.get_barrier_semaphore()
    for step in range(1, 16):
        pl.semaphore_signal(barrier, inc=1, **to(lax.rem(me + step, 16)))

    turn[0] = jnp.concatenate([cos_ref[...], cos_ref[...]], axis=1)
    turn[1] = jnp.concatenate([-sin_ref[...], sin_ref[...]], axis=1)
    gain = gain_ref[...].astype(jnp.float32)[None, :]

    x_in.wait()

    def a_copy(r):
        rows = pl.ds(pl.multiple_of(core * OWN + r * LAG, LAG), LAG)
        return pltpu.make_async_remote_copy(a_s.at[rows, :], a_s.at[rows, :], a_send.at[r], a_recv.at[r], **to(partner))

    for r in range(OWN // LAG):
        wide = y_ref[r * LAG : (r + 1) * LAG, :].astype(jnp.float32)
        scale = lax.rsqrt(jnp.mean(wide * wide, -1, keepdims=True) + 1e-6)
        rows = pl.ds(pl.multiple_of(core * OWN + r * LAG, LAG), LAG)
        a_s[rows, :] = (wide * scale * gain).astype(jnp.bfloat16)
        if r == 0:
            pl.semaphore_wait(barrier, 15)
        else:
            a_copy(r - 1).start()
    a_copy(OWN // LAG - 1).start()
    for r in range(OWN // LAG):
        rows = pl.ds(pl.multiple_of((1 - core) * OWN + r * LAG, LAG), LAG)
        pltpu.make_async_remote_copy(a_s.at[rows, :], a_s.at[rows, :], a_send.at[r], a_recv.at[r], **to(partner)).wait_recv()

    def place(m, ref, half, slot):
        if m == 1:
            return vstage.at[slot, half * W : (half + 1) * W, :], vt_s.at[:, pl.ds(pl.multiple_of(ref * TOK, TOK), TOK)]
        return (stage.at[slot, :, half * W : (half + 1) * W], (k_s, None, q_s)[m].at[pl.ds(pl.multiple_of(ref * TOK, TOK), TOK), :])

    def send(p):
        slot = lax.rem(p, 2)
        t = _xor(chip, _mask(core, p))
        for m in range(3):
            @pl.when((p >= 4 * m) & (p < 4 * m + 4))
            def _():
                for half in range(2):
                    src, dst = place(m, chip, half, slot)
                    owner = 2 * t + half

                    @pl.when(owner == me)
                    def _():
                        pltpu.make_async_copy(src, dst, s_recv.at[m, chip]).start()

                    @pl.when(owner != me)
                    def _():
                        pltpu.make_async_remote_copy(src, dst, s_send.at[slot, half], s_recv.at[m, chip], **to(owner)).start()

    def sent(p):
        slot = lax.rem(p, 2)
        t = _xor(chip, _mask(core, p))
        for half in range(2):
            @pl.when(2 * t + half != me)
            def _():
                src, dst = place(0, chip, half, slot)
                pltpu.make_async_remote_copy(src, dst, s_send.at[slot, half], s_recv.at[0, chip], **to(partner)).wait_send()

            @pl.when(2 * t + half == me)
            def _():
                for m in range(3):
                    @pl.when((p >= 4 * m) & (p < 4 * m + 4))
                    def _():
                        src, dst = place(m, chip, half, slot)
                        pltpu.make_async_copy(src, dst, s_recv.at[m, chip]).wait()

    def group(p, _):
        slot = lax.rem(p, 2)
        for kc in range(KB):
            i = p * KB + kc
            d = jnp.dot(a_s[:, kc * BLK : (kc + 1) * BLK], arrived(i), preferred_element_type=jnp.float32)
            if kc:
                acc[0] = acc[0] + d
            else:
                acc[0] = d
            fetch(i + RING)
            if kc == 0:
                @pl.when(p > 0)
                def _():
                    send(p - 1)

        @pl.when(p > 1)
        def _():
            sent(p - 2)

        @pl.when(lax.div(p, 4) != 1)
        def _():
            for h in range(2 * HEADS):
                cols = slice(h * HEAD, (h + 1) * HEAD)
                t = acc[0, :, cols].astype(jnp.bfloat16).astype(jnp.float32)
                stage[slot, :, cols] = (t * turn[0] + pltpu.roll(t, HEAD // 2, 1) * turn[1]).astype(jnp.bfloat16)

        @pl.when(lax.div(p, 4) == 1)
        def _():
            for h in range(2 * HEADS):
                cols = slice(h * HEAD, (h + 1) * HEAD)
                vstage[slot, cols, :] = acc[0, :, cols].T.astype(jnp.bfloat16)

    lax.fori_loop(0, GROUPS, group, None)
    send(jnp.int32(GROUPS - 1))
    for r in range(OWN // LAG):
        a_copy(r).wait_send()

    def received(m, c):
        @pl.when((c != chip) | (lax.rem(core + m, 2) == 1))
        def _():
            src, dst = place(m, c, 0, 0)
            pltpu.make_async_remote_copy(src, dst, s_send.at[0, 0], s_recv.at[m, c], **to(partner)).wait_recv()

    def keys_and_values(c, _):
        received(0, c)
        received(1, c)

    lax.fori_loop(0, CHIPS, keys_and_values, None)

    def o_copy(iq):
        rows = pl.ds(pl.multiple_of(iq * TOK, TOK), TOK)
        return pltpu.make_async_remote_copy(q_s.at[rows, :], seen.at[chip], o_send.at[iq], o_recv.at[chip], **to(2 * iq + core))

    def own_copy():
        rows = pl.ds(pl.multiple_of(chip * TOK, TOK), TOK)
        return pltpu.make_async_copy(q_s.at[rows, :], seen.at[chip], o_send.at[chip])

    def queries(k, _):
        iq = _xor(chip, _pick(ORDER, k))
        received(2, iq)
        attend_block(q_s, k_s, vt_s, top_s, mix_s, iq)

        @pl.when(iq != chip)
        def _():
            o_copy(iq).start()

        @pl.when(iq == chip)
        def _():
            own_copy().start()

    lax.fori_loop(0, CHIPS, queries, None)

    sent(jnp.int32(GROUPS - 2))
    sent(jnp.int32(GROUPS - 1))

    def p_copy(n):
        rows = pl.ds(pl.multiple_of((1 - core) * OWN, OWN), OWN)
        return pltpu.make_async_remote_copy(acc.at[n, rows, :], other.at[lax.rem(n, 2)], p_send.at[n], p_recv.at[n], **to(partner))

    def finish(n):
        cols = pl.ds(pl.multiple_of(n * BLK, BLK), BLK)
        p_copy(n).wait_recv()
        mine = acc[n, pl.ds(pl.multiple_of(core * OWN, OWN), OWN), :]
        y_ref[:, cols] = (y_ref[:, cols].astype(jnp.float32) + (mine + other[lax.rem(n, 2)])).astype(jnp.bfloat16)

    def arrival(k):
        c = _xor(chip, TERMS[k])
        if TERMS[k]:
            pltpu.make_async_remote_copy(seen.at[c], seen.at[c], o_send.at[c], o_recv.at[c], **to(partner)).wait_recv()
        else:
            own_copy().wait()

    def add(i, n, b):
        terms = jnp.concatenate([seen[_xor(chip, TERMS[2 * b])], seen[_xor(chip, TERMS[2 * b + 1])]], axis=1)
        d = jnp.dot(terms, arrived(i), preferred_element_type=jnp.float32)
        if b:
            acc[n] = acc[n] + d
        else:
            acc[n] = d
        fetch(i + RING)

    first = GROUPS * KB
    for b in range(2):
        arrival(2 * b)
        arrival(2 * b + 1)
        lax.fori_loop(0, OUTS, lambda n, _: add(first + b * OUTS + n, n, b), None)
    for k in range(4, 6):
        arrival(k)

    def ending(n, _):
        add(first + 2 * (OUTS + n), n, 2)

        @pl.when(n > 0)
        def _():
            finish(n - 1)

        @pl.when(n == 0)
        def _():
            for k in range(6, 8):
                arrival(k)

        add(first + 2 * (OUTS + n) + 1, n, 3)
        p_copy(n).start()

    lax.fori_loop(0, OUTS, ending, None)
    finish(jnp.int32(OUTS - 1))
    for n in range(OUTS):
        p_copy(jnp.int32(n)).wait_send()

    def drain(c, _):
        @pl.when(c != chip)
        def _():
            o_copy(c).wait_send()

    lax.fori_loop(0, CHIPS, drain, None)


def solution(mesh):
    def step(x, gain, wq, wk, wv, wo):
        me = lax.axis_index("sp")
        place = lax.div(me, 2) * TOK + jnp.arange(TOK)
        half = HEAD // 2
        angle = place.astype(jnp.float32)[:, None] * THETA ** (-jnp.arange(half, dtype=jnp.float32) / half)
        cos, sin = jnp.cos(angle), jnp.sin(angle)
        vmem, hbm = pl.BlockSpec(memory_space=pltpu.VMEM), pl.BlockSpec(memory_space=pl.ANY)
        return pl.pallas_call(
            layer,
            out_shape=pltpu.VMEM((OWN, D), jnp.bfloat16),
            in_specs=[hbm, vmem, vmem, vmem, hbm, hbm, hbm, hbm],
            out_specs=vmem,
            scratch_shapes=[
                pltpu.VMEM((TOK, D), jnp.bfloat16),
                pltpu.VMEM((SEQ, W), jnp.bfloat16),
                pltpu.VMEM((SEQ, W), jnp.bfloat16),
                pltpu.VMEM((W, SEQ), jnp.bfloat16),
                pltpu.VMEM((RING, BLK, BLK), jnp.bfloat16),
                pltpu.VMEM((OUTS, TOK, BLK), jnp.float32),
                pltpu.VMEM((2, TOK, BLK), jnp.bfloat16),
                pltpu.VMEM((2, BLK, TOK), jnp.bfloat16),
                pltpu.VMEM((CHIPS, TOK, W), jnp.bfloat16),
                pltpu.VMEM((2, OWN, BLK), jnp.float32),
                pltpu.VMEM((2, TOK, HEAD), jnp.float32),
                pltpu.VMEM((8, TOK), jnp.float32),
                pltpu.VMEM((HEADS, HEAD + 8, TOK), jnp.float32),
                pltpu.SemaphoreType.DMA((RING,)),
                pltpu.SemaphoreType.DMA,
                pltpu.SemaphoreType.DMA((OWN // LAG,)),
                pltpu.SemaphoreType.DMA((OWN // LAG,)),
                pltpu.SemaphoreType.DMA((2, 2)),
                pltpu.SemaphoreType.DMA((3, CHIPS)),
                pltpu.SemaphoreType.DMA((CHIPS,)),
                pltpu.SemaphoreType.DMA((CHIPS,)),
                pltpu.SemaphoreType.DMA((OUTS,)),
                pltpu.SemaphoreType.DMA((OUTS,)),
            ],
            compiler_params=pltpu.CompilerParams(collective_id=0, has_side_effects=True, vmem_limit_bytes=VMEM),
            cost_estimate=pl.CostEstimate(flops=160 * 10**9, bytes_accessed=61 * 10**7, transcendentals=15 * 10**6),
        )(x, gain, cos, sin, wq, wk, wv, wo)

    tokens, whole = P(("dp", "sp"), None), P(None, None)
    return jax.shard_map(
        step,
        mesh=mesh,
        in_specs=(tokens, P(None), whole, whole, whole, whole),
        out_specs=tokens,
        check_vma=False,
    )
```
